32 devices in a mesh: grp: 2 (over core), gx: 4 (over y, x), gy: 4 (over z).
Axes of the slice: x: 2, y: 2, z: 4, core: 2. Of those that a mesh axis runs over, the one named last changes fastest.
Arguments:
- coarse_density: float32 [512, 512, 512], P('gx', ('grp', 'gy')), may hold values from -3 to 3
- fine_density: float32 [32, 128, 256], P('gx', 'gy', 'grp'), may hold values from -96 to 96
- fine_start: float32 [32, 128, 256], P('gx', 'gy', 'grp'), may hold values from -6 to 6
- anchor: int32 [3], replicated, may hold values from 1 to 447
Outputs:
- coarse_potential: float32 [512, 512, 512], P('gx', ('grp', 'gy'))
- fine_potential: float32 [32, 128, 256], P('gx', 'gy', 'grp')
The draws below stay inside these ranges and needn't reach their ends.
Inputs may be any that keep to these rules, and one draw needn't show every extreme that they name: Along every dimension d the coarse cells anchor[d] - 1 up to anchor[d] + (fine cells along d) / 4 lie inside the coarse grid.
All inputs are finite; a program needn't handle non-finite values.
Results may differ from the reference program's by a relative error of at most 0.00015.
Values sent between devices are 32-bit elements; how exact they have to be, the bound alone decides.
A program may use at most 128 MiB of HBM per device.

```python
import math
import jax
import jax.numpy as jnp
from jax import lax

NC = 512
RATIO = 4
SWEEPS = 8
FX = 32
FY = 128
FZ = 256
CBX = 10
CBY = 34
CBZ = 66


def block_levels(rng, shape, pieces, low, high):
    def one(dim, parts):
        steps = jax.random.uniform(jax.random.fold_in(jax.random.fold_in(rng, 6), dim), (parts,), jnp.float32, low / len(pieces), high / len(pieces))
        return jnp.repeat(jnp.exp(steps), shape[dim] // parts).reshape((-1,) + (1,) * (len(shape) - dim - 1))

    factor_of = one(*pieces[0])
    for cut in pieces[1:]:
        factor_of = factor_of * one(*cut)
    return factor_of


def gaussian(key, extent, width, reach, cuts=(), kind=jnp.bfloat16):
    values = width * jax.random.normal(key, extent, jnp.float32)
    if cuts:
        values = values * block_levels(key, extent, cuts, -0.22, 0.18)
    return jnp.clip(values, -reach, reach).astype(kind)


def setup_inputs(seed: int = 0) -> dict:
    key_list = jax.random.split(jax.random.key(seed), 5)
    coarse_density = gaussian(key_list[0], (NC, NC, NC), 0.5, 3.0, ((0, 4), (1, 8)), jnp.float32)
    fine_density = gaussian(key_list[1], (FX, FY, FZ), 16.0, 96.0, ((0, 4), (1, 4), (2, 2)), jnp.float32)
    fine_start = gaussian(key_list[2], (FX, FY, FZ), 1.0, 6.0, ((0, 4), (1, 4), (2, 2)), jnp.float32)
    anchor = jax.random.randint(key_list[3], (3,), 1, NC - max(FX, max(FY, FZ)) // RATIO).astype(jnp.int32)
    return dict(coarse_density=coarse_density, fine_density=fine_density, fine_start=fine_start, anchor=anchor)


highest = lax.Precision.HIGHEST

def sine_table(amount):
    indices = jnp.arange(amount, dtype=jnp.int32) + 1
    product = indices[:, None] * indices[None, :] % (2 * (amount + 1))
    angles = product.astype(jnp.float32) * (math.pi / (amount + 1))
    return math.sqrt(2.0 / (amount + 1)) * jnp.sin(angles)

def eigen_values(indices, amount):
    angles = (indices + 1).astype(jnp.float32) * (math.pi / (2 * (amount + 1)))
    return -4.0 * jnp.square(jnp.sin(angles))

def interpolation(fine_index, cell_count):
    scaled = 2 * fine_index + 1 + RATIO
    bottom = scaled // (2 * RATIO)
    weight = (scaled % (2 * RATIO)).astype(jnp.float32) / (2.0 * RATIO)
    column = jnp.arange(cell_count, dtype=jnp.int32)
    first_part = jnp.where(column[None, :] == bottom[:, None], 1.0 - weight[:, None], 0.0)
    second_part = jnp.where(column[None, :] == bottom[:, None] + 1, weight[:, None], 0.0)
    return first_part + second_part

def transform(values, matrix):
    values = jnp.einsum('abc,cd->abd', values, matrix, precision=highest)
    values = jnp.einsum('abc,bd->adc', values, matrix, precision=highest)
    return jnp.einsum('abc,ad->dbc', values, matrix, precision=highest)

def ghost_values(face, left_matrix, right_matrix):
    partial_value = jnp.einsum('fbc,kc->fbk', face, right_matrix, precision=highest)
    return jnp.einsum('fbk,jb->fjk', partial_value, left_matrix, precision=highest)

def reference(coarse_density, fine_density, fine_start, anchor):
    matrix = sine_table(NC)
    eigen_list = eigen_values(jnp.arange(NC, dtype=jnp.int32), NC)
    spectrum = transform(coarse_density, matrix)
    divisor = eigen_list[:, None, None] + eigen_list[None, :, None] + eigen_list[None, None, :]
    potential = transform(spectrum / divisor, matrix)
    coarse_box = lax.dynamic_slice(potential, (anchor[0] - 1, anchor[1] - 1, anchor[2] - 1), (CBX, CBY, CBZ))
    ends_x = interpolation(jnp.array([-1, FX], dtype=jnp.int32), CBX)
    ends_y = interpolation(jnp.array([-1, FY], dtype=jnp.int32), CBY)
    ends_z = interpolation(jnp.array([-1, FZ], dtype=jnp.int32), CBZ)
    inner_x = interpolation(jnp.arange(FX, dtype=jnp.int32), CBX)
    inner_y = interpolation(jnp.arange(FY, dtype=jnp.int32), CBY)
    inner_z = interpolation(jnp.arange(FZ, dtype=jnp.int32), CBZ)
    face_x = jnp.einsum('fa,abc->fbc', ends_x, coarse_box, precision=highest)
    face_y = jnp.einsum('fb,abc->fac', ends_y, coarse_box, precision=highest)
    face_z = jnp.einsum('fc,abc->fab', ends_z, coarse_box, precision=highest)
    ghost_x = ghost_values(face_x, inner_y, inner_z)
    ghost_y = ghost_values(face_y, inner_x, inner_z)
    ghost_z = ghost_values(face_z, inner_x, inner_y)
    padded = jnp.zeros((FX + 2, FY + 2, FZ + 2), jnp.float32)
    padded = padded.at[1:-1, 1:-1, 1:-1].set(fine_start)
    padded = padded.at[0, 1:-1, 1:-1].set(ghost_x[0]).at[-1, 1:-1, 1:-1].set(ghost_x[1])
    padded = padded.at[1:-1, 0, 1:-1].set(ghost_y[0]).at[1:-1, -1, 1:-1].set(ghost_y[1])
    padded = padded.at[1:-1, 1:-1, 0].set(ghost_z[0]).at[1:-1, 1:-1, -1].set(ghost_z[1])
    source = fine_density / (RATIO * RATIO)
    for sweep in range(SWEEPS):
        summed = padded[2:, 1:-1, 1:-1] + padded[:-2, 1:-1, 1:-1]
        summed = summed + padded[1:-1, 2:, 1:-1] + padded[1:-1, :-2, 1:-1]
        summed = summed + padded[1:-1, 1:-1, 2:] + padded[1:-1, 1:-1, :-2]
        padded = padded.at[1:-1, 1:-1, 1:-1].set((summed - source) / 6.0)
    return (potential, padded[1:-1, 1:-1, 1:-1])
```

```python
import math

import jax
import jax.numpy as jnp
from jax import lax
from jax.sharding import PartitionSpec as P

RATIO = 4
SWEEPS = 8
EVERY = ("gx", "grp", "gy")

highest = lax.Precision.HIGHEST
high = lax.Precision.HIGH


def with_halo(block, sides, width):
    for axis, dim in sides:
        count = lax.axis_size(axis)
        forward = [(i, i + 1) for i in range(count - 1)]
        backward = [(target, source) for source, target in forward]
        low = lax.ppermute(
            lax.slice_in_dim(block, block.shape[dim] - width, None, axis=dim), axis, forward
        )
        high_side = lax.ppermute(lax.slice_in_dim(block, 0, width, axis=dim), axis, backward)
        block = jnp.concatenate([low, block, high_side], axis=dim)
    return block


def sine_table(amount):
    indices = jnp.arange(amount, dtype=jnp.int32) + 1
    product = indices[:, None] * indices[None, :] % (2 * (amount + 1))
    angles = product.astype(jnp.float32) * (math.pi / (amount + 1))
    return math.sqrt(2.0 / (amount + 1)) * jnp.sin(angles)


def eigen_values(indices, amount):
    angles = (indices + 1).astype(jnp.float32) * (math.pi / (2 * (amount + 1)))
    return -4.0 * jnp.square(jnp.sin(angles))


def interpolation(fine_index, cell_count):
    scaled = 2 * fine_index + 1 + RATIO
    bottom = scaled // (2 * RATIO)
    weight = (scaled % (2 * RATIO)).astype(jnp.float32) / (2.0 * RATIO)
    column = jnp.arange(cell_count, dtype=jnp.int32)
    first_part = jnp.where(column[None, :] == bottom[:, None], 1.0 - weight[:, None], 0.0)
    second_part = jnp.where(column[None, :] == bottom[:, None] + 1, weight[:, None], 0.0)
    return first_part + second_part


def ghost_values(face, left_matrix, right_matrix):
    partial_value = jnp.einsum("fbc,kc->fbk", face, right_matrix, precision=highest)
    return jnp.einsum("fbk,jb->fjk", partial_value, left_matrix, precision=highest)


def neighbours(padded):
    summed = padded[2:, 1:-1, 1:-1] + padded[:-2, 1:-1, 1:-1]
    summed = summed + padded[1:-1, 2:, 1:-1] + padded[1:-1, :-2, 1:-1]
    return summed + padded[1:-1, 1:-1, 2:] + padded[1:-1, 1:-1, :-2]


def swap_sides(planes):
    inner = planes[1:-1].reshape((-1, 2) + planes.shape[1:])[:, ::-1]
    inner = inner.reshape((-1,) + planes.shape[1:])
    zero = jnp.zeros_like(planes[:1])
    return jnp.concatenate([zero, inner, zero], axis=0)


def coarse_solve(density):
    rows, cols, depth = density.shape
    strips = lax.axis_size("gx")
    bands = lax.axis_size(("grp", "gy"))
    devices = strips * bands
    share = depth // devices
    length_0 = rows * strips
    length_1 = cols * bands
    sine_0 = sine_table(rows)
    sine_1 = sine_table(cols)
    sine_2 = sine_table(depth)
    full_0 = sine_table(length_0)
    full_1 = full_0 if length_1 == length_0 else sine_table(length_1)
    eigen_2 = eigen_values(jnp.arange(depth, dtype=jnp.int32), depth)
    local = (
        eigen_values(jnp.arange(rows, dtype=jnp.int32), rows)[:, None, None]
        + eigen_values(jnp.arange(cols, dtype=jnp.int32), cols)[None, :, None]
        + eigen_2[None, None, :]
    )
    wide_1 = jnp.broadcast_to(sine_1[None], (rows, cols, cols))

    def first(block):
        return jnp.einsum("da,abc->dbc", sine_0, block, precision=high)

    def second(block):
        return jnp.einsum("adb,abc->adc", wide_1, block, precision=high)

    def third(block):
        return jnp.einsum("abc,cd->abd", block, sine_2, precision=high)

    spectrum = first(second(third(density)))
    alone = spectrum / local
    ends_0 = jnp.stack([sine_0[0], sine_0[-1]])
    ends_1 = jnp.stack([sine_1[0], sine_1[-1]])
    trace_0 = jnp.einsum("ea,abc->ebc", ends_0, alone, precision=highest)
    trace_0 = jnp.einsum("ebc,bd->edc", trace_0, sine_1, precision=highest)
    trace_1 = jnp.einsum("eb,abc->eac", ends_1, alone, precision=highest)
    trace_1 = jnp.einsum("eac,ad->edc", trace_1, sine_0, precision=highest)
    cut = 2 * cols
    packed = jnp.concatenate(
        [trace_0.reshape(cut, depth), trace_1.reshape(2 * rows, depth)], axis=0
    )
    packed = packed.T.reshape(devices, share, cut + 2 * rows)
    packed = lax.all_to_all(packed, EVERY, split_axis=0, concat_axis=0, tiled=True)
    planes_0 = packed[:, :, :cut].reshape(strips, bands, share, 2, cols)
    planes_0 = planes_0.transpose(0, 3, 2, 1, 4).reshape(2 * strips, share, length_1)
    planes_1 = packed[:, :, cut:].reshape(strips, bands, share, 2, rows)
    planes_1 = planes_1.transpose(1, 3, 2, 0, 4).reshape(2 * bands, share, length_0)
    source_0 = jnp.einsum("pkj,jl->kpl", -swap_sides(planes_0), full_1, precision=highest)
    source_1 = jnp.einsum("qkj,jl->kql", -swap_sides(planes_1), full_0, precision=highest)
    sides_0 = full_0.reshape(strips, rows, length_0)[:, jnp.array([0, rows - 1])]
    sides_0 = sides_0.reshape(2 * strips, length_0)
    sides_1 = full_1.reshape(bands, cols, length_1)[:, jnp.array([0, cols - 1])]
    sides_1 = sides_1.reshape(2 * bands, length_1)
    wide_sides_0 = jnp.broadcast_to(sides_0[None], (share,) + sides_0.shape)
    wide_sides_1 = jnp.broadcast_to(sides_1[None], (share,) + sides_1.shape)
    left = jnp.concatenate([wide_sides_0, source_1], axis=1)
    right = jnp.concatenate([source_0, wide_sides_1], axis=1)
    mine = lax.axis_index(EVERY) * share + jnp.arange(share, dtype=jnp.int32)
    whole = (
        eigen_values(mine, depth)[:, None, None]
        + eigen_values(jnp.arange(length_0, dtype=jnp.int32), length_0)[None, :, None]
        + eigen_values(jnp.arange(length_1, dtype=jnp.int32), length_1)[None, None, :]
    )
    wave = jnp.einsum("kpa,kpb->kab", left, right, precision=highest) / whole
    wave_0 = jnp.einsum("kpa,kab->kpb", wide_sides_0, wave, precision=highest)
    wave_1 = jnp.einsum("kqb,kab->kqa", wide_sides_1, wave, precision=highest)
    side_0 = planes_0 + jnp.einsum("kpl,jl->pkj", wave_0, full_1, precision=highest)
    side_1 = planes_1 + jnp.einsum("kql,jl->qkj", wave_1, full_0, precision=highest)
    back_0 = swap_sides(side_0).reshape(strips, 2, share, bands, cols)
    back_0 = back_0.transpose(0, 3, 2, 1, 4).reshape(devices, share, cut)
    back_1 = swap_sides(side_1).reshape(bands, 2, share, strips, rows)
    back_1 = back_1.transpose(3, 0, 2, 1, 4).reshape(devices, share, 2 * rows)
    back = jnp.concatenate([back_0, back_1], axis=2)
    back = lax.all_to_all(back, EVERY, split_axis=0, concat_axis=0, tiled=True)
    back = back.reshape(depth, cut + 2 * rows).T
    bound_0 = back[:cut].reshape(2, cols, depth)
    bound_1 = back[cut:].reshape(2, rows, depth)
    bound_0 = jnp.einsum("ebc,bd->edc", bound_0, sine_1, precision=highest)
    bound_1 = jnp.einsum("eac,ad->edc", bound_1, sine_0, precision=highest)
    known = sum(
        ends_0[e][:, None, None] * bound_0[e][None, :, :]
        + ends_1[e][None, :, None] * bound_1[e][:, None, :]
        for e in range(2)
    )
    return third(second(first((spectrum - known) / local)))


def box_faces(potential, anchor, ends, bounds):
    rows, cols, depth = potential.shape
    ends_x, ends_y, ends_z = ends
    bound_x, bound_y, bound_z = bounds
    near_x = min(bound_x, rows)
    near_y = min(bound_y, cols)
    shift_x = anchor[0] - 1 - lax.axis_index("gx") * rows
    shift_y = anchor[1] - 1 - lax.axis_index(("grp", "gy")) * cols
    from_x = jnp.clip(shift_x, 0, rows - near_x)
    from_y = jnp.clip(shift_y, 0, cols - near_y)
    piece = lax.dynamic_slice(
        potential, (from_x, from_y, anchor[2] - 1), (near_x, near_y, bound_z)
    )

    def place(start, near, shift, bound):
        here = start + jnp.arange(near, dtype=jnp.int32)
        window = shift + jnp.arange(bound, dtype=jnp.int32)
        return (window[:, None] == here[None, :]).astype(jnp.float32)

    piece = jnp.einsum("ax,xyz->ayz", place(from_x, near_x, shift_x, bound_x), piece, precision=highest)
    box = jnp.einsum("by,ayz->abz", place(from_y, near_y, shift_y, bound_y), piece, precision=highest)
    face_x = jnp.einsum("fa,abc->fbc", ends_x, box, precision=highest)
    face_y = jnp.einsum("fb,abc->fac", ends_y, box, precision=highest)
    face_z = jnp.einsum("fc,abc->fab", ends_z, box, precision=highest)
    return lax.psum((face_x, face_y, face_z), ("grp", "gx", "gy"))


def body(coarse_density, fine_density, fine_start, anchor):
    fine_rows, fine_cols, fine_depth = fine_start.shape
    total_x = fine_rows * lax.axis_size("gx")
    total_y = fine_cols * lax.axis_size("gy")
    total_z = fine_depth * lax.axis_size("grp")
    bounds = tuple(total // RATIO + 2 for total in (total_x, total_y, total_z))
    width = min(SWEEPS, fine_rows, fine_cols, fine_depth)
    sides = (("gx", 0), ("gy", 1), ("grp", 2))
    density = with_halo(fine_density, sides, width)
    values = with_halo(fine_start, sides, width)

    potential = coarse_solve(coarse_density)
    ends = tuple(
        interpolation(jnp.array([-1, total], dtype=jnp.int32), bound)
        for total, bound in zip((total_x, total_y, total_z), bounds)
    )
    face_x, face_y, face_z = box_faces(potential, anchor, ends, bounds)
    index_x = lax.axis_index("gx") * fine_rows - width + jnp.arange(fine_rows + 2 * width, dtype=jnp.int32)
    index_y = lax.axis_index("gy") * fine_cols - width + jnp.arange(fine_cols + 2 * width, dtype=jnp.int32)
    index_z = lax.axis_index("grp") * fine_depth - width + jnp.arange(fine_depth + 2 * width, dtype=jnp.int32)
    inner_x = interpolation(index_x, bounds[0])
    inner_y = interpolation(index_y, bounds[1])
    inner_z = interpolation(index_z, bounds[2])
    ghost_x = ghost_values(face_x, inner_y, inner_z)
    ghost_y = ghost_values(face_y, inner_x, inner_z)
    ghost_z = ghost_values(face_z, inner_x, inner_y)
    at_x = index_x[:, None, None]
    at_y = index_y[None, :, None]
    at_z = index_z[None, None, :]
    boundary = jnp.where(at_x == 0, ghost_x[0][None], 0.0)
    boundary = boundary + jnp.where(at_x == total_x - 1, ghost_x[1][None], 0.0)
    boundary = boundary + jnp.where(at_y == 0, ghost_y[0][:, None, :], 0.0)
    boundary = boundary + jnp.where(at_y == total_y - 1, ghost_y[1][:, None, :], 0.0)
    boundary = boundary + jnp.where(at_z == 0, ghost_z[0][:, :, None], 0.0)
    boundary = boundary + jnp.where(at_z == total_z - 1, ghost_z[1][:, :, None], 0.0)
    inside = (at_x >= 0) & (at_x < total_x) & (at_y >= 0) & (at_y < total_y)
    inside = inside & (at_z >= 0) & (at_z < total_z)
    source = boundary - density / (RATIO * RATIO)
    left = width
    for sweep in range(SWEEPS):
        if left == 0:
            values = with_halo(values, sides, width)
            left = width
        margin = width - left + 1
        trim = tuple(slice(margin, size - margin) for size in source.shape)
        values = (neighbours(values) + source[trim]) / 6.0
        values = jnp.where(inside[trim], values, 0.0)
        left -= 1
    if left:
        values = values[left:-left, left:-left, left:-left]
    return (potential, values)


def solution(mesh):
    return jax.shard_map(
        body,
        mesh=mesh,
        in_specs=(P("gx", ("grp", "gy"), None), P("gx", "gy", "grp"), P("gx", "gy", "grp"), P()),
        out_specs=(P("gx", ("grp", "gy"), None), P("gx", "gy", "grp")),
        check_vma=False,
    )
```
